32 devices in a mesh: space: 16 (over z, y, core), tm: 2 (over x).
Axes of the slice: x: 2, y: 2, z: 4, core: 2. Of those that a mesh axis runs over, the one named last changes fastest.
Arguments:
- row_orbitals: bfloat16 [8192, 2048], P('space', 'tm'), may hold values from -0.890625 to 0.890625
- column_orbitals: bfloat16 [256, 2048], P('space', 'tm'), may hold values from -0.890625 to 0.890625
- occupation: int32 [2048], replicated, may hold values from 0 to 2
- order: int32 [2048], replicated, may hold values from 0 to 2047, each once
- levels: float32 [2048], replicated, may hold values from 0.1 to 1
- times: float32 [2], replicated, may hold values from 0.05 to 1.5
- quad_weights: float32 [2], replicated, may hold values from 0.5 to 1.5
- freqs: float32 [8], replicated, may hold values from 0.1 to 4
Outputs:
- spectrum: float32 [8, 8192, 256], P(None, ('space', 'tm'))
The draws below stay inside these ranges and needn't reach their ends.
Inputs may be any that keep to these rules, and one draw needn't show every extreme that they name: `order`: each index of 0 to 2047 once.
All inputs are finite; a program needn't handle non-finite values.
Results may differ from the reference program's by a relative error of at most 0.0026.
Values may be sent and summed in bfloat16 or wider, within the bound.
No kernel may reach another device: no remote copies, remote signals or barrier semaphores. Data moves between devices by JAX's collectives and lax.ppermute only.
A program may use at most 64 MiB of HBM per device.

```python
import math
import jax
import jax.numpy as jnp
from jax import lax

NORB = 2048
NFREQ = 8
NTIME = 2
NROW = 8192
NCOL = 256


def set_ends(array, key, low, top_value):
    dims = array.shape
    place = [jax.random.randint(jax.random.fold_in(key, axis), (), 0, dims[axis]) for axis in range(len(dims))]
    array = array.at[tuple(place)].set(low)
    longest = dims.index(max(dims))
    place[longest] = (place[longest] + 1) % dims[longest]
    return array.at[tuple(place)].set(top_value)


def block_scale(own_key, dims, shards, low, largest):
    loudness, own = 1.0, jax.random.fold_in(own_key, 6)
    for axis_at, parts in shards:
        heights = jnp.exp(jax.random.uniform(jax.random.fold_in(own, axis_at), (parts,), jnp.float32, low / len(shards), largest / len(shards)))
        loudness = loudness * jnp.repeat(heights, dims[axis_at] // parts).reshape([-1 if axis == axis_at else 1 for axis in range(len(dims))])
    return loudness


def noise(stream_key, shape, deviation, bound, cuts=(), held_as=jnp.bfloat16):
    array = jax.random.normal(stream_key, shape, jnp.float32) * deviation
    if len(cuts) > 0:
        array = block_scale(stream_key, shape, cuts, -0.22, 0.18) * array
    return jnp.clip(array, min=-bound, max=bound).astype(held_as)


def setup_inputs(seed: int = 0) -> dict:
    seeds = jax.random.split(jax.random.key(seed), 9)
    return {
        "row_orbitals": noise(seeds[0], (NROW, NORB), (NORB ** -0.25), 0.890625, ((0, 16), (1, 2))),
        "column_orbitals": noise(seeds[1], (NCOL, NORB), (NORB ** -0.25), 0.890625, ((0, 16), (1, 2))),
        "occupation": set_ends(jax.random.randint(seeds[2], (NORB,), 0, 3), jax.random.fold_in(seeds[2], 1), 0, 2).astype(jnp.int32),
        "order": jax.random.permutation(seeds[3], NORB).astype(jnp.int32),
        "levels": jnp.clip(jnp.exp(jax.random.uniform(seeds[4], (NORB,), jnp.float32, math.log(0.1), math.log(1.0))), 0.1, 1.0),
        "times": jnp.clip(jnp.exp(jax.random.uniform(seeds[5], (NTIME,), jnp.float32, math.log(0.05), math.log(1.5))), 0.05, 1.5),
        "quad_weights": jnp.clip(jax.random.uniform(seeds[6], (NTIME,), jnp.float32, 0.5, 1.5), 0.5, 1.5),
        "freqs": jnp.clip(jnp.exp(jax.random.uniform(seeds[7], (NFREQ,), jnp.float32, math.log(0.1), math.log(4.0))), 0.1, 4.0),
    }


def reference(row_orbitals, column_orbitals, occupation, order, levels, times, quad_weights, freqs):
    energy = jnp.take(levels, order.astype(jnp.int32))
    filled = occupation.astype(jnp.float32) * 0.5
    cosines = quad_weights[None, :] * jnp.cos(freqs[:, None] * times[None, :])
    columns = column_orbitals.astype(jnp.float32)
    row_values = row_orbitals.astype(jnp.float32)
    spectrum = jnp.zeros((NFREQ, NROW, NCOL), jnp.float32)
    for which in range(NTIME):
        decays = jnp.exp(-times[which] * energy)
        scaled_full = lax.optimization_barrier((row_values * (filled * decays)[None, :]).astype(jnp.bfloat16)).astype(jnp.float32)
        scaled_empty = lax.optimization_barrier((row_values * ((1.0 - filled) * decays)[None, :]).astype(jnp.bfloat16)).astype(jnp.float32)
        green_full = jnp.dot(scaled_full, columns.T, precision=lax.Precision.HIGHEST)
        green_empty = jnp.dot(scaled_empty, columns.T, precision=lax.Precision.HIGHEST)
        polar = lax.optimization_barrier((green_full * green_empty).astype(jnp.bfloat16)).astype(jnp.float32)
        spectrum = spectrum + cosines[:, which][:, None, None] * polar[None]
    return spectrum
```

```python
import functools

import jax
import jax.numpy as jnp
from jax import lax
from jax.experimental import pallas as pl
from jax.experimental.pallas import tpu as pltpu
from jax.sharding import PartitionSpec as P


LANES = 128
MIB = 1 << 20
VMEM = pl.BlockSpec(memory_space=pltpu.VMEM)
ANY = pl.BlockSpec(memory_space=pl.ANY)


def scale_rows(read, scaled_ref, decay_ref, first_page):
    times = decay_ref.shape[0]
    block = scaled_ref.shape[0] // times
    for q in range(scaled_ref.shape[1] // LANES):
        lanes = pl.ds(q * LANES, LANES)
        values = read(lanes).astype(jnp.float32)
        for j in range(times):
            weight = decay_ref[j, pl.ds(first_page + q, 1), :]
            scaled_ref[pl.ds(j * block, block), lanes] = (values * weight).astype(jnp.bfloat16)


def own_kernel(rows_ref, levels_ref, page_ref, lane_ref, times_ref, scaled_ref, decay_ref):
    page, lane = page_ref[...], lane_ref[...]
    energy = jnp.zeros(page.shape, jnp.float32)
    for p in range(page.shape[0]):
        row = jnp.broadcast_to(levels_ref[pl.ds(p, 1), :], page.shape)
        energy = jnp.where(page == p, jnp.take_along_axis(row, lane, axis=1), energy)
    for j in range(times_ref.shape[0]):
        decay_ref[j] = jnp.exp(times_ref[pl.ds(j, 1), :] * energy)
    me = lax.axis_index("tm")
    scale_rows(lambda lanes: rows_ref[:, lanes], scaled_ref, decay_ref, me * (rows_ref.shape[1] // LANES))


def other_kernel(bits, rows_ref, decay_ref, scaled_ref):
    me = lax.axis_index("tm")
    scale_rows(lambda lanes: rows_ref[:, lanes], scaled_ref, decay_ref, (me ^ bits) * (rows_ref.shape[1] // LANES))


def half_kernel(layout, tm, far, *refs):
    pieces, refs = refs[: len(layout)], refs[len(layout) :]
    scaled, refs = refs[:tm], refs[tm:]
    occupation_ref, cosines_ref, *rest = refs
    out_ref, weights, greens, stage, sems = rest[-5:]
    block = stage.shape[1]
    width = scaled[0].shape[1]
    times = scaled[0].shape[0] // block
    columns = stage.shape[2]
    points = pieces[0].shape[-2]
    pages = width // LANES
    me = lax.axis_index("tm")
    here = lax.axis_index("space")
    peers = columns // points
    for h in range(tm):
        for q in range(pages):
            lanes = pl.ds(h * width + q * LANES, LANES)
            full = occupation_ref[pl.ds((me ^ h) * pages + q, 1), :].astype(jnp.float32) * 0.5
            empty = (1.0 - full).astype(jnp.bfloat16)
            full = full.astype(jnp.bfloat16)
            for ref, owners in zip(pieces, layout):
                for i, owner in enumerate(owners):
                    values = ref[:, lanes] if len(ref.shape) == 2 else ref[i, :, lanes]
                    start = pl.multiple_of(((here ^ owner) % peers) * points, points)
                    weights[pl.ds(start, points), lanes] = values * full
                    weights[pl.ds(columns + start, points), lanes] = values * empty

    for h in range(tm):
        part = lax.dot_general(
            scaled[h][...],
            weights[:, h * width : (h + 1) * width],
            (((1,), (1,)), ((), ())),
            preferred_element_type=jnp.float32,
        )
        greens[...] = part if h == 0 else greens[...] + part

    steps = sems.shape[0]
    rows = block // steps
    side = (here // peers) ^ far
    target = pl.ds(pl.multiple_of(side * columns, LANES), columns)
    copies = []
    for s in range(steps):
        at = pl.ds(s * rows, rows)
        polar = []
        for j in range(times):
            both = greens[pl.ds(j * block + s * rows, rows), :]
            polar.append((both[:, :columns] * both[:, columns:]).astype(jnp.bfloat16).astype(jnp.float32))
        for k in range(stage.shape[0]):
            value = cosines_ref[pl.ds(k * times, 1), :] * polar[0]
            for j in range(1, times):
                value += cosines_ref[pl.ds(k * times + j, 1), :] * polar[j]
            stage[k, at, :] = value
        copies.append(pltpu.make_async_copy(stage.at[:, at, :], out_ref.at[:, at, target], sems.at[s]))
        copies[-1].start()
    for copy in copies:
        copy.wait()


def body(row_orbitals, column_orbitals, occupation, order, levels, times, quad_weights, freqs):
    tm, space = lax.axis_size("tm"), lax.axis_size("space")
    lines = space // 4
    width = row_orbitals.shape[1]
    block = row_orbitals.shape[0] // tm
    time_count, freq_count = times.shape[0], freqs.shape[0]
    me = lax.axis_index("tm")

    def swap(value, axis, bits):
        size = lax.axis_size(axis)
        return lax.ppermute(value, axis, [(i, i ^ bits) for i in range(size)])

    halves = [column_orbitals] + [swap(column_orbitals, "tm", h) for h in range(1, tm)]
    others = [swap(lax.dynamic_slice_in_dim(row_orbitals, (me ^ h) * block, block, 0), "tm", h) for h in range(1, tm)]
    unit = jnp.concatenate(halves, axis=1)
    held = {0: unit}
    for k in range(1, lines):
        held[4 * k] = swap(unit, "space", 4 * k)
    for k in range(lines):
        held[4 * k + 2] = swap(held[4 * k], "space", 2)
    sides = [[o for o in held if o < space // 2], [o for o in held if o >= space // 2]]
    twins = [swap(jnp.stack([held[o] for o in side]), "space", 1) for side in sides]

    pages = (-1, LANES)
    small = pltpu.CompilerParams(vmem_limit_bytes=8 * MIB)
    table = (levels.shape[0] // LANES, LANES)
    own_scaled, decays = pl.pallas_call(
        own_kernel,
        out_shape=(
            jax.ShapeDtypeStruct((time_count * block, width), jnp.bfloat16),
            jax.ShapeDtypeStruct((time_count, *table), jnp.float32),
        ),
        in_specs=[VMEM] * 5,
        out_specs=(VMEM,) * 2,
        compiler_params=small,
        name="own",
    )(
        lax.dynamic_slice_in_dim(row_orbitals, me * block, block, 0),
        -levels.reshape(pages),
        (order // LANES).reshape(pages),
        (order % LANES).reshape(pages),
        jnp.broadcast_to(times[:, None], (time_count, LANES)),
    )

    scaled = [own_scaled]
    for h, rows in enumerate(others, 1):
        scaled.append(
            pl.pallas_call(
                functools.partial(other_kernel, h),
                out_shape=jax.ShapeDtypeStruct(own_scaled.shape, jnp.bfloat16),
                in_specs=[VMEM] * 2,
                out_specs=VMEM,
                compiler_params=small,
            )(rows, decays)
        )
    columns = unit.shape[0] * space // 2
    cosines = quad_weights[None, :] * jnp.cos(freqs[:, None] * times[None, :])
    cosines = jnp.broadcast_to(cosines.reshape(-1, 1), (freq_count * time_count, columns))
    steps = 4
    spectrum = []
    for i, side in enumerate(sides):
        arrays = [held[o] for o in side] + [twins[i]]
        layout = [[o] for o in side] + [[o ^ 1 for o in side]]
        count = len(arrays) + tm + 2
        spectrum = [
            pl.pallas_call(
                functools.partial(half_kernel, layout, tm, i),
                out_shape=jax.ShapeDtypeStruct((freq_count, block, 2 * columns), jnp.float32),
                in_specs=[VMEM] * count + [ANY] * len(spectrum),
                out_specs=ANY,
                scratch_shapes=[
                    pltpu.VMEM((2 * columns, tm * width), jnp.bfloat16),
                    pltpu.VMEM((time_count * block, 2 * columns), jnp.float32),
                    pltpu.VMEM((freq_count, block, columns), jnp.float32),
                    pltpu.SemaphoreType.DMA((steps,)),
                ],
                input_output_aliases={count: 0} if spectrum else {},
                compiler_params=pltpu.CompilerParams(vmem_limit_bytes=20 * MIB),
            )(*arrays, *scaled, occupation.reshape(pages), cosines, *spectrum)
        ]
    return spectrum[0]


def solution(mesh):
    placed = (P("space", "tm"), P("space", "tm"), P(), P(), P(), P(), P(), P())
    return jax.shard_map(body, mesh=mesh, in_specs=placed, out_specs=P(None, ("space", "tm"), None), check_vma=False)
```

```python
import functools

import jax
import jax.numpy as jnp
from jax import lax
from jax.experimental import pallas as pl
from jax.experimental.pallas import tpu as pltpu
from jax.sharding import PartitionSpec as P


LANES = 128
STORES = 4
MIB = 1 << 20
VMEM = pl.BlockSpec(memory_space=pltpu.VMEM)
ANY = pl.BlockSpec(memory_space=pl.ANY)


def scale_rows(rows_ref, scaled_ref, decay_ref, first_page):
    block = rows_ref.shape[0]
    for q in range(scaled_ref.shape[1] // LANES):
        lanes = pl.ds(q * LANES, LANES)
        values = rows_ref[:, lanes].astype(jnp.float32)
        for j in range(decay_ref.shape[0]):
            weight = decay_ref[j, pl.ds(first_page + q, 1), :]
            scaled_ref[pl.ds(j * block, block), lanes] = (values * weight).astype(jnp.bfloat16)


def own_kernel(rows_ref, levels_ref, page_ref, lane_ref, times_ref, scaled_ref, decay_ref):
    page, lane = page_ref[...], lane_ref[...]
    energy = jnp.zeros(page.shape, jnp.float32)
    for p in range(page.shape[0]):
        row = jnp.broadcast_to(levels_ref[pl.ds(p, 1), :], page.shape)
        energy = jnp.where(page == p, jnp.take_along_axis(row, lane, axis=1), energy)
    for j in range(times_ref.shape[0]):
        decay_ref[j] = jnp.exp(times_ref[pl.ds(j, 1), :] * energy)
    me = lax.axis_index("tm")
    scale_rows(rows_ref, scaled_ref, decay_ref, me * (rows_ref.shape[1] // LANES))


def other_kernel(bits, rows_ref, decay_ref, scaled_ref):
    me = lax.axis_index("tm")
    scale_rows(rows_ref, scaled_ref, decay_ref, (me ^ bits) * (rows_ref.shape[1] // LANES))


def products(layout, tm, pieces, scaled, occupation_ref, weights, columns):
    width = scaled[0].shape[1]
    points = pieces[0].shape[-2]
    pages = width // LANES
    me = lax.axis_index("tm")
    here = lax.axis_index("space")
    for h in range(tm):
        for q in range(pages):
            lanes = pl.ds(q * LANES, LANES)
            source = pl.ds(h * width + q * LANES, LANES)
            full = occupation_ref[pl.ds((me ^ h) * pages + q, 1), :].astype(jnp.float32) * 0.5
            empty = (1.0 - full).astype(jnp.bfloat16)
            full = full.astype(jnp.bfloat16)
            for ref, owners in zip(pieces, layout):
                for i, owner in enumerate(owners):
                    values = ref[:, source] if len(ref.shape) == 2 else ref[i, :, source]
                    place = (here ^ owner ^ (h > 0)) % (columns // points)
                    start = pl.multiple_of(place * points, points)
                    weights[h][pl.ds(start, points), lanes] = values * full
                    weights[h][pl.ds(columns + start, points), lanes] = values * empty
    greens = None
    for h in range(tm):
        product = lax.dot_general(
            scaled[h][...], weights[h][...], (((1,), (1,)), ((), ())), preferred_element_type=jnp.float32
        )
        greens = product if h == 0 else greens + product
    return greens


def polar_of(greens, columns):
    return (greens[:, :columns] * greens[:, columns:]).astype(jnp.bfloat16)


def transform(read_polar, side, times, cosines_ref, out_ref, stage, sems):
    block, columns = stage.shape[1:]
    some = block // sems.shape[0]
    target = pl.ds(pl.multiple_of(side * columns, LANES), columns)
    copies = []
    for i in range(sems.shape[0]):
        at = pl.ds(i * some, some)
        polar = [read_polar(j * block + i * some, some).astype(jnp.float32) for j in range(times)]
        for k in range(stage.shape[0]):
            value = cosines_ref[pl.ds(k * times, 1), :] * polar[0]
            for j in range(1, times):
                value += cosines_ref[pl.ds(k * times + j, 1), :] * polar[j]
            stage[k, at, :] = value
        copies.append(pltpu.make_async_copy(stage.at[:, at, :], out_ref.at[:, at, target], sems.at[i]))
        copies[-1].start()
    return copies


def near_kernel(layout, tm, *refs):
    pieces, scaled = refs[: len(layout)], refs[len(layout) : len(layout) + tm]
    occupation_ref, polar_ref, *weights = refs[len(layout) + tm :]
    columns = polar_ref.shape[1]
    polar_ref[...] = polar_of(products(layout, tm, pieces, scaled, occupation_ref, weights, columns), columns)


def far_kernel(layout, tm, *refs):
    pieces, scaled = refs[: len(layout)], refs[len(layout) : len(layout) + tm]
    polar_ref, occupation_ref, cosines_ref, out_ref, *weights = refs[len(layout) + tm : -4]
    stages, sems = refs[-4:-2], refs[-2:]
    block, columns = stages[0].shape[1:]
    times = polar_ref.shape[0] // block
    space = lax.axis_size("space")
    side = lax.axis_index("space") // (space // 2)
    copies = transform(
        lambda at, size: polar_ref[pl.ds(at, size), :], side, times, cosines_ref, out_ref, stages[0], sems[0]
    )
    greens = products(layout, tm, pieces, scaled, occupation_ref, weights, columns)
    copies += transform(
        lambda at, size: polar_of(greens[at : at + size], columns),
        1 - side, times, cosines_ref, out_ref, stages[1], sems[1],
    )
    for copy in copies:
        copy.wait()


def body(row_orbitals, column_orbitals, occupation, order, levels, times, quad_weights, freqs):
    tm, space = lax.axis_size("tm"), lax.axis_size("space")
    lines = space // 4
    width = row_orbitals.shape[1]
    block = row_orbitals.shape[0] // tm
    time_count, freq_count = times.shape[0], freqs.shape[0]
    me = lax.axis_index("tm")

    def swap(value, bits, h=0):
        pairs = [(s * tm + t, (s ^ bits) * tm + (t ^ h)) for s in range(space) for t in range(tm)]
        return lax.ppermute(value, ("space", "tm"), pairs)

    halves = [column_orbitals] + [swap(column_orbitals, 1, h) for h in range(1, tm)]
    others = [swap(lax.dynamic_slice_in_dim(row_orbitals, (me ^ h) * block, block, 0), 0, h) for h in range(1, tm)]
    unit = jnp.concatenate(halves, axis=1)
    held = {0: unit}
    middle = lines // 2
    for k in range(1, middle + 1):
        held[4 * k + 1] = swap(unit, 4 * k + 1)
    base = held[4 * middle + 1]
    for k in range(1, middle):
        held[4 * (middle + k)] = swap(base, 4 * k + 1)
    for o, value in list(held.items()):
        held[o ^ 3] = swap(value, 3)
    last = list(held)[-1]
    groups = [[o for o in held if o < space // 2], [o for o in held if o >= space // 2 and o != last], [last]]
    twins = []
    for group in groups:
        stack = jnp.stack([held[o] for o in group]) if len(group) > 1 else held[group[0]]
        twins.append(swap(stack, 1))

    pages = (-1, LANES)
    small = pltpu.CompilerParams(vmem_limit_bytes=8 * MIB)
    table = (levels.shape[0] // LANES, LANES)
    own_scaled, decays = pl.pallas_call(
        own_kernel,
        out_shape=(
            jax.ShapeDtypeStruct((time_count * block, width), jnp.bfloat16),
            jax.ShapeDtypeStruct((time_count, *table), jnp.float32),
        ),
        in_specs=[VMEM] * 5,
        out_specs=(VMEM,) * 2,
        compiler_params=small,
        name="own",
    )(
        lax.dynamic_slice_in_dim(row_orbitals, me * block, block, 0),
        -levels.reshape(pages),
        (order // LANES).reshape(pages),
        (order % LANES).reshape(pages),
        jnp.broadcast_to(times[:, None], (time_count, LANES)),
    )

    scaled = [own_scaled]
    for h, rows in enumerate(others, 1):
        scaled.append(
            pl.pallas_call(
                functools.partial(other_kernel, h),
                out_shape=jax.ShapeDtypeStruct(own_scaled.shape, jnp.bfloat16),
                in_specs=[VMEM] * 2,
                out_specs=VMEM,
                compiler_params=small,
            )(rows, decays)
        )
    columns = unit.shape[0] * space // 2
    cosines = quad_weights[None, :] * jnp.cos(freqs[:, None] * times[None, :])
    cosines = jnp.broadcast_to(cosines.reshape(-1, 1), (freq_count * time_count, columns))
    layouts, arrays = [], []
    for side in (0, 1):
        mine = [i for i in range(len(groups)) if (i > 0) == side]
        layouts.append([[o] for i in mine for o in groups[i]] + [[o ^ 1 for o in groups[i]] for i in mine])
        arrays.append([held[o] for i in mine for o in groups[i]] + [twins[i] for i in mine])
    weights = [pltpu.VMEM((2 * columns, width), jnp.bfloat16)] * tm
    stage = pltpu.VMEM((freq_count, block, columns), jnp.float32)
    staging = [stage, stage, pltpu.SemaphoreType.DMA((2,)), pltpu.SemaphoreType.DMA((STORES,))]
    result = jax.ShapeDtypeStruct((freq_count, block, 2 * columns), jnp.float32)
    large = pltpu.CompilerParams(vmem_limit_bytes=20 * MIB)
    occupation = occupation.reshape(pages)
    polar = pl.pallas_call(
        functools.partial(near_kernel, layouts[0], tm),
        out_shape=jax.ShapeDtypeStruct((time_count * block, columns), jnp.bfloat16),
        in_specs=[VMEM] * (len(arrays[0]) + tm + 1),
        out_specs=VMEM,
        scratch_shapes=weights,
        compiler_params=large,
        name="near",
    )(*arrays[0], *scaled, occupation)
    return pl.pallas_call(
        functools.partial(far_kernel, layouts[1], tm),
        out_shape=result,
        in_specs=[VMEM] * (len(arrays[1]) + tm + 3),
        out_specs=ANY,
        scratch_shapes=weights + staging,
        compiler_params=large,
        name="far",
    )(*arrays[1], *scaled, polar, occupation, cosines)


def solution(mesh):
    placed = (P("space", "tm"), P("space", "tm"), P(), P(), P(), P(), P(), P())
    return jax.shard_map(body, mesh=mesh, in_specs=placed, out_specs=P(None, ("space", "tm"), None), check_vma=False)
```

```python
import functools

import jax
import jax.numpy as jnp
from jax import lax
from jax.experimental import pallas as pl
from jax.experimental.pallas import tpu as pltpu
from jax.sharding import PartitionSpec as P


LANES = 128
STORES = 4
MIB = 1 << 20
VMEM = pl.BlockSpec(memory_space=pltpu.VMEM)
ANY = pl.BlockSpec(memory_space=pl.ANY)


def scale_rows(rows_ref, scaled_ref, decay_ref, first_page):
    block = rows_ref.shape[0]
    for q in range(scaled_ref.shape[1] // LANES):
        lanes = pl.ds(q * LANES, LANES)
        values = rows_ref[:, lanes].astype(jnp.float32)
        for j in range(decay_ref.shape[0]):
            weight = decay_ref[j, pl.ds(first_page + q, 1), :]
            scaled_ref[pl.ds(j * block, block), lanes] = (values * weight).astype(jnp.bfloat16)


def own_kernel(rows_ref, levels_ref, page_ref, lane_ref, times_ref, scaled_ref, decay_ref):
    page, lane = page_ref[...], lane_ref[...]
    energy = jnp.zeros(page.shape, jnp.float32)
    for p in range(page.shape[0]):
        row = jnp.broadcast_to(levels_ref[pl.ds(p, 1), :], page.shape)
        energy = jnp.where(page == p, jnp.take_along_axis(row, lane, axis=1), energy)
    for j in range(times_ref.shape[0]):
        decay_ref[j] = jnp.exp(times_ref[pl.ds(j, 1), :] * energy)
    me = lax.axis_index("tm")
    scale_rows(rows_ref, scaled_ref, decay_ref, me * (rows_ref.shape[1] // LANES))


def other_kernel(bits, rows_ref, decay_ref, scaled_ref):
    me = lax.axis_index("tm")
    scale_rows(rows_ref, scaled_ref, decay_ref, (me ^ bits) * (rows_ref.shape[1] // LANES))


def products(layout, tm, pieces, scaled, occupation_ref, weights, columns):
    width = scaled[0].shape[1]
    points = pieces[0].shape[-2]
    pages = width // LANES
    me = lax.axis_index("tm")
    here = lax.axis_index("space")
    greens = None
    for h in range(tm):
        for q in range(pages):
            lanes = pl.ds(q * LANES, LANES)
            source = pl.ds(h * width + q * LANES, LANES)
            full = occupation_ref[pl.ds((me ^ h) * pages + q, 1), :].astype(jnp.float32) * 0.5
            empty = (1.0 - full).astype(jnp.bfloat16)
            full = full.astype(jnp.bfloat16)
            for ref, owners in zip(pieces, layout):
                for i, owner in enumerate(owners):
                    values = ref[:, source] if len(ref.shape) == 2 else ref[i, :, source]
                    place = (here ^ owner ^ (h > 0)) % (columns // points)
                    start = pl.multiple_of(place * points, points)
                    weights[h][pl.ds(start, points), lanes] = values * full
                    weights[h][pl.ds(columns + start, points), lanes] = values * empty
        product = lax.dot_general(
            scaled[h][...], weights[h][...], (((1,), (1,)), ((), ())), preferred_element_type=jnp.float32
        )
        greens = product if h == 0 else greens + product
    return greens


def polar_of(greens, columns):
    return (greens[:, :columns] * greens[:, columns:]).astype(jnp.bfloat16)


def transform(read_polar, times, cosines_ref, stage, at, some):
    block = stage.shape[1]
    polar = [read_polar(j * block + at, some).astype(jnp.float32) for j in range(times)]
    for k in range(stage.shape[0]):
        value = cosines_ref[pl.ds(k * times, 1), :] * polar[0]
        for j in range(1, times):
            value += cosines_ref[pl.ds(k * times + j, 1), :] * polar[j]
        stage[k, pl.ds(at, some), :] = value


def near_kernel(layout, tm, *refs):
    pieces, scaled = refs[: len(layout)], refs[len(layout) : len(layout) + tm]
    occupation_ref, cosines_ref, stage, *weights = refs[len(layout) + tm :]
    block, columns = stage.shape[1:]
    greens = products(layout, tm, pieces, scaled, occupation_ref, weights, columns)
    times = greens.shape[0] // block
    transform(lambda at, size: polar_of(greens[at : at + size], columns), times, cosines_ref, stage, 0, block)


def far_kernel(layout, tm, *refs):
    pieces, scaled = refs[: len(layout)], refs[len(layout) : len(layout) + tm]
    near_ref, occupation_ref, cosines_ref, out_ref, *weights = refs[len(layout) + tm : -3]
    stage, near_sem, sems = refs[-3:]
    block, columns = stage.shape[1:]
    space = lax.axis_size("space")
    side = lax.axis_index("space") // (space // 2)

    def target(which):
        return pl.ds(pl.multiple_of(which * columns, LANES), columns)

    copies = [pltpu.make_async_copy(near_ref, out_ref.at[:, :, target(side)], near_sem)]
    copies[0].start()
    greens = products(layout, tm, pieces, scaled, occupation_ref, weights, columns)
    times = greens.shape[0] // block
    some = block // sems.shape[0]
    for i in range(sems.shape[0]):
        transform(
            lambda at, size: polar_of(greens[at : at + size], columns), times, cosines_ref, stage, i * some, some
        )
        rows = pl.ds(i * some, some)
        copies.append(pltpu.make_async_copy(stage.at[:, rows, :], out_ref.at[:, rows, target(1 - side)], sems.at[i]))
        copies[-1].start()
    for copy in copies:
        copy.wait()


def body(row_orbitals, column_orbitals, occupation, order, levels, times, quad_weights, freqs):
    tm, space = lax.axis_size("tm"), lax.axis_size("space")
    lines = space // 4
    width = row_orbitals.shape[1]
    block = row_orbitals.shape[0] // tm
    time_count, freq_count = times.shape[0], freqs.shape[0]
    me = lax.axis_index("tm")

    def swap(value, bits, h=0):
        pairs = [(s * tm + t, (s ^ bits) * tm + (t ^ h)) for s in range(space) for t in range(tm)]
        return lax.ppermute(value, ("space", "tm"), pairs)

    halves = [column_orbitals] + [swap(column_orbitals, 1, h) for h in range(1, tm)]
    others = [swap(lax.dynamic_slice_in_dim(row_orbitals, (me ^ h) * block, block, 0), 0, h) for h in range(1, tm)]
    unit = jnp.concatenate(halves, axis=1)
    held = {0: unit}
    middle = lines // 2
    for k in range(1, middle + 1):
        held[4 * k + 1] = swap(unit, 4 * k + 1)
    base = held[4 * middle + 1]
    for k in range(1, middle):
        held[4 * (middle + k)] = swap(base, 4 * k + 1)
    for o, value in list(held.items()):
        held[o ^ 3] = swap(value, 3)
    last = list(held)[-1]
    groups = [[o for o in held if o < space // 2], [o for o in held if o >= space // 2 and o != last], [last]]
    twins = []
    for group in groups:
        stack = jnp.stack([held[o] for o in group]) if len(group) > 1 else held[group[0]]
        twins.append(swap(stack, 1))

    pages = (-1, LANES)
    small = pltpu.CompilerParams(vmem_limit_bytes=8 * MIB)
    table = (levels.shape[0] // LANES, LANES)
    own_scaled, decays = pl.pallas_call(
        own_kernel,
        out_shape=(
            jax.ShapeDtypeStruct((time_count * block, width), jnp.bfloat16),
            jax.ShapeDtypeStruct((time_count, *table), jnp.float32),
        ),
        in_specs=[VMEM] * 5,
        out_specs=(VMEM,) * 2,
        compiler_params=small,
        name="own",
    )(
        lax.dynamic_slice_in_dim(row_orbitals, me * block, block, 0),
        -levels.reshape(pages),
        (order // LANES).reshape(pages),
        (order % LANES).reshape(pages),
        jnp.broadcast_to(times[:, None], (time_count, LANES)),
    )

    scaled = [own_scaled]
    for h, rows in enumerate(others, 1):
        scaled.append(
            pl.pallas_call(
                functools.partial(other_kernel, h),
                out_shape=jax.ShapeDtypeStruct(own_scaled.shape, jnp.bfloat16),
                in_specs=[VMEM] * 2,
                out_specs=VMEM,
                compiler_params=small,
            )(rows, decays)
        )
    columns = unit.shape[0] * space // 2
    cosines = quad_weights[None, :] * jnp.cos(freqs[:, None] * times[None, :])
    cosines = jnp.broadcast_to(cosines.reshape(-1, 1), (freq_count * time_count, columns))
    layouts, arrays = [], []
    for side in (0, 1):
        mine = [i for i in range(len(groups)) if (i > 0) == side]
        layouts.append([[o] for i in mine for o in groups[i]] + [[o ^ 1 for o in groups[i]] for i in mine])
        arrays.append([held[o] for i in mine for o in groups[i]] + [twins[i] for i in mine])
    weights = [pltpu.VMEM((2 * columns, width), jnp.bfloat16)] * tm
    staging = [
        pltpu.VMEM((freq_count, block, columns), jnp.float32),
        pltpu.SemaphoreType.DMA,
        pltpu.SemaphoreType.DMA((STORES,)),
    ]
    result = jax.ShapeDtypeStruct((freq_count, block, 2 * columns), jnp.float32)
    large = pltpu.CompilerParams(vmem_limit_bytes=20 * MIB)
    occupation = occupation.reshape(pages)
    near = pl.pallas_call(
        functools.partial(near_kernel, layouts[0], tm),
        out_shape=jax.ShapeDtypeStruct((freq_count, block, columns), jnp.float32),
        in_specs=[VMEM] * (len(arrays[0]) + tm + 2),
        out_specs=VMEM,
        scratch_shapes=weights,
        compiler_params=large,
        name="near",
    )(*arrays[0], *scaled, occupation, cosines)
    return pl.pallas_call(
        functools.partial(far_kernel, layouts[1], tm),
        out_shape=result,
        in_specs=[VMEM] * (len(arrays[1]) + tm + 3),
        out_specs=ANY,
        scratch_shapes=weights + staging,
        compiler_params=large,
        name="far",
    )(*arrays[1], *scaled, near, occupation, cosines)


def solution(mesh):
    placed = (P("space", "tm"), P("space", "tm"), P(), P(), P(), P(), P(), P())
    return jax.shard_map(body, mesh=mesh, in_specs=placed, out_specs=P(None, ("space", "tm"), None), check_vma=False)
```

```python
import functools

import jax
import jax.numpy as jnp
from jax import lax
from jax.experimental import pallas as pl
from jax.experimental.pallas import tpu as pltpu
from jax.sharding import PartitionSpec as P


LANES = 128
STORES = 4
MIB = 1 << 20
VMEM = pl.BlockSpec(memory_space=pltpu.VMEM)
ANY = pl.BlockSpec(memory_space=pl.ANY)


def scale_rows(rows_ref, scaled_ref, decay_ref, first_page):
    block = rows_ref.shape[0]
    for q in range(scaled_ref.shape[1] // LANES):
        lanes = pl.ds(q * LANES, LANES)
        values = rows_ref[:, lanes].astype(jnp.float32)
        for j in range(decay_ref.shape[0]):
            weight = decay_ref[j, pl.ds(first_page + q, 1), :]
            scaled_ref[pl.ds(j * block, block), lanes] = (values * weight).astype(jnp.bfloat16)


def own_kernel(rows_ref, levels_ref, page_ref, lane_ref, times_ref, scaled_ref, decay_ref):
    page, lane = page_ref[...], lane_ref[...]
    energy = jnp.zeros(page.shape, jnp.float32)
    for p in range(page.shape[0]):
        row = jnp.broadcast_to(levels_ref[pl.ds(p, 1), :], page.shape)
        energy = jnp.where(page == p, jnp.take_along_axis(row, lane, axis=1), energy)
    for j in range(times_ref.shape[0]):
        decay_ref[j] = jnp.exp(times_ref[pl.ds(j, 1), :] * energy)
    me = lax.axis_index("tm")
    scale_rows(rows_ref, scaled_ref, decay_ref, me * (rows_ref.shape[1] // LANES))


def other_kernel(bits, rows_ref, decay_ref, scaled_ref):
    me = lax.axis_index("tm")
    scale_rows(rows_ref, scaled_ref, decay_ref, (me ^ bits) * (rows_ref.shape[1] // LANES))


def products(layout, tm, pieces, scaled, occupation_ref, weights, columns):
    width = scaled[0].shape[1]
    points = pieces[0].shape[-2]
    pages = width // LANES
    me = lax.axis_index("tm")
    here = lax.axis_index("space")
    greens = None
    for h in range(tm):
        for q in range(pages):
            lanes = pl.ds(q * LANES, LANES)
            source = pl.ds(h * width + q * LANES, LANES)
            full = occupation_ref[pl.ds((me ^ h) * pages + q, 1), :].astype(jnp.float32) * 0.5
            empty = (1.0 - full).astype(jnp.bfloat16)
            full = full.astype(jnp.bfloat16)
            for ref, owners in zip(pieces, layout):
                for i, owner in enumerate(owners):
                    values = ref[:, source] if len(ref.shape) == 2 else ref[i, :, source]
                    place = (here ^ owner ^ (h > 0)) % (columns // points)
                    start = pl.multiple_of(place * points, points)
                    weights[h][pl.ds(start, points), lanes] = values * full
                    weights[h][pl.ds(columns + start, points), lanes] = values * empty
        product = lax.dot_general(
            scaled[h][...], weights[h][...], (((1,), (1,)), ((), ())), preferred_element_type=jnp.float32
        )
        greens = product if h == 0 else greens + product
    return greens


def polar_of(greens, columns):
    return (greens[:, :columns] * greens[:, columns:]).astype(jnp.bfloat16)


def transform(read_polar, times, cosines_ref, stage, at, some):
    block = stage.shape[1]
    polar = [read_polar(j * block + at, some).astype(jnp.float32) for j in range(times)]
    for k in range(stage.shape[0]):
        value = cosines_ref[pl.ds(k * times, 1), :] * polar[0]
        for j in range(1, times):
            value += cosines_ref[pl.ds(k * times + j, 1), :] * polar[j]
        stage[k, pl.ds(at, some), :] = value


def near_kernel(layout, tm, *refs):
    pieces, scaled = refs[: len(layout)], refs[len(layout) : len(layout) + tm]
    occupation_ref, cosines_ref, stage, *weights = refs[len(layout) + tm :]
    block, columns = stage.shape[1:]
    greens = products(layout, tm, pieces, scaled, occupation_ref, weights, columns)
    times = greens.shape[0] // block
    transform(lambda at, size: polar_of(greens[at : at + size], columns), times, cosines_ref, stage, 0, block)


def far_kernel(layout, tm, *refs):
    pieces, scaled = refs[: len(layout)], refs[len(layout) : len(layout) + tm]
    near_ref, occupation_ref, cosines_ref, out_ref, *weights = refs[len(layout) + tm : -3]
    stage, near_sem, sems = refs[-3:]
    block, columns = stage.shape[1:]
    space = lax.axis_size("space")
    side = lax.axis_index("space") // (space // 2)

    def target(which):
        return pl.ds(pl.multiple_of(which * columns, LANES), columns)

    copies = [pltpu.make_async_copy(near_ref, out_ref.at[:, :, target(side)], near_sem)]
    copies[0].start()
    greens = products(layout, tm, pieces, scaled, occupation_ref, weights, columns)
    times = greens.shape[0] // block
    some = block // sems.shape[0]
    for i in range(sems.shape[0]):
        transform(
            lambda at, size: polar_of(greens[at : at + size], columns), times, cosines_ref, stage, i * some, some
        )
        rows = pl.ds(i * some, some)
        copies.append(pltpu.make_async_copy(stage.at[:, rows, :], out_ref.at[:, rows, target(1 - side)], sems.at[i]))
        copies[-1].start()
    for copy in copies:
        copy.wait()


def body(row_orbitals, column_orbitals, occupation, order, levels, times, quad_weights, freqs):
    tm, space = lax.axis_size("tm"), lax.axis_size("space")
    lines = space // 4
    width = row_orbitals.shape[1]
    block = row_orbitals.shape[0] // tm
    time_count, freq_count = times.shape[0], freqs.shape[0]
    me = lax.axis_index("tm")

    def swap(value, bits, h=0):
        pairs = [(s * tm + t, (s ^ bits) * tm + (t ^ h)) for s in range(space) for t in range(tm)]
        return lax.ppermute(value, ("space", "tm"), pairs)

    halves = [column_orbitals] + [swap(column_orbitals, 1, h) for h in range(1, tm)]
    others = [swap(lax.dynamic_slice_in_dim(row_orbitals, (me ^ h) * block, block, 0), 0, h) for h in range(1, tm)]
    unit = jnp.concatenate(halves, axis=1)
    held = {0: unit}
    middle = lines // 2
    for k in range(1, middle + 1):
        held[4 * k + 1] = swap(unit, 4 * k + 1)
    base = held[4 * middle + 1]
    for k in range(1, middle):
        held[4 * (middle + k)] = swap(base, 4 * k + 1)
    for o, value in list(held.items()):
        held[o ^ 3] = swap(value, 3)
    last = list(held)[-1]
    groups = [[o for o in held if o < space // 2], [o for o in held if o >= space // 2 and o != last], [last]]
    twins = []
    for group in groups:
        stack = jnp.stack([held[o] for o in group]) if len(group) > 1 else held[group[0]]
        twins.append(swap(stack, 1))

    pages = (-1, LANES)
    small = pltpu.CompilerParams(vmem_limit_bytes=8 * MIB)
    table = (levels.shape[0] // LANES, LANES)
    tables = -levels.reshape(pages), (order // LANES).reshape(pages), (order % LANES).reshape(pages)
    own_scaled, decays = pl.pallas_call(
        own_kernel,
        out_shape=(
            jax.ShapeDtypeStruct((time_count * block, width), jnp.bfloat16),
            jax.ShapeDtypeStruct((time_count, *table), jnp.float32),
        ),
        in_specs=[VMEM] * 5,
        out_specs=(VMEM,) * 2,
        compiler_params=small,
        name="own",
    )(
        lax.dynamic_slice_in_dim(lax.optimization_barrier((row_orbitals, unit))[0], me * block, block, 0),
        *tables,
        jnp.broadcast_to(times[:, None], (time_count, LANES)),
    )

    scaled = [own_scaled]
    for h, rows in enumerate(others, 1):
        scaled.append(
            pl.pallas_call(
                functools.partial(other_kernel, h),
                out_shape=jax.ShapeDtypeStruct(own_scaled.shape, jnp.bfloat16),
                in_specs=[VMEM] * 2,
                out_specs=VMEM,
                compiler_params=small,
            )(rows, decays)
        )
    columns = unit.shape[0] * space // 2
    cosines = quad_weights[None, :] * jnp.cos(freqs[:, None] * times[None, :])
    cosines = jnp.broadcast_to(cosines.reshape(-1, 1), (freq_count * time_count, columns))
    layouts, arrays = [], []
    for side in (0, 1):
        mine = [i for i in range(len(groups)) if (i > 0) == side]
        layouts.append([[o] for i in mine for o in groups[i]] + [[o ^ 1 for o in groups[i]] for i in mine])
        arrays.append([held[o] for i in mine for o in groups[i]] + [twins[i] for i in mine])
    weights = [pltpu.VMEM((2 * columns, width), jnp.bfloat16)] * tm
    staging = [
        pltpu.VMEM((freq_count, block, columns), jnp.float32),
        pltpu.SemaphoreType.DMA,
        pltpu.SemaphoreType.DMA((STORES,)),
    ]
    result = jax.ShapeDtypeStruct((freq_count, block, 2 * columns), jnp.float32)
    large = pltpu.CompilerParams(vmem_limit_bytes=20 * MIB)
    occupation = occupation.reshape(pages)
    near = pl.pallas_call(
        functools.partial(near_kernel, layouts[0], tm),
        out_shape=jax.ShapeDtypeStruct((freq_count, block, columns), jnp.float32),
        in_specs=[VMEM] * (len(arrays[0]) + tm + 2),
        out_specs=VMEM,
        scratch_shapes=weights,
        compiler_params=large,
        name="near",
    )(*arrays[0], *scaled, occupation, cosines)
    return pl.pallas_call(
        functools.partial(far_kernel, layouts[1], tm),
        out_shape=result,
        in_specs=[VMEM] * (len(arrays[1]) + tm + 3),
        out_specs=ANY,
        scratch_shapes=weights + staging,
        compiler_params=large,
        name="far",
    )(*arrays[1], *scaled, near, occupation, cosines)


def solution(mesh):
    placed = (P("space", "tm"), P("space", "tm"), P(), P(), P(), P(), P(), P())
    return jax.shard_map(body, mesh=mesh, in_specs=placed, out_specs=P(None, ("space", "tm"), None), check_vma=False)
```
